512 devices in a mesh: node: 32 (over y, x, core), row: 16 (over z).
Axes of the slice: x: 4, y: 4, z: 16, core: 2. Of those that a mesh axis runs over, the one named last changes fastest.
Arguments:
- samples: bfloat16 [32, 16384, 384], P('node', 'row'), parts along dimension 0, may hold values from -6 to 6
- column_order: int32 [32, 384], P('node'), parts along dimension 0, may hold values from 0 to 383, each once within a row
- skeleton: int32 [32, 256], P('node'), parts along dimension 0, may hold values from 0 to 16383, as said below
Outputs:
- q_factor: float32 [32, 16384, 384], P('node', 'row'), parts along dimension 0
- interp: bfloat16 [32, 16384, 256], P('node', 'row'), parts along dimension 0
The draws below stay inside these ranges and needn't reach their ends.
There are 32 independent parts, one for each index of `node`. The reference program is written for one: setup_inputs(seed, part) draws one part's arguments, and reference() takes and returns one part's arrays. A program takes and returns all parts, laid end to end along the dimension named above; each array names one. Nothing has to cross between parts.
Inputs may be any that keep to these rules, and one draw needn't show every extreme that they name: `skeleton`: each row names 256 distinct sample rows in ascending order. `column_order`: each row is a permutation.
All inputs are finite; a program needn't handle non-finite values.
Results may differ from the reference program's by a relative error of at most 0.001.
Values sent between devices are 32-bit elements; how exact they have to be, the bound alone decides.
A program may use at most 64 MiB of HBM per device.

```python
import jax
import jax.numpy as jnp
from jax import lax

C = 384
K = 256
ROWS_DEV = 1024
FRONTS = 1
ROWS = 16384
N_ROW = 16


def draw_skeleton(key, part):
    keys = jax.random.split(jax.random.fold_in(key, 7), FRONTS)

    def pick(single):
        return jnp.sort(jax.random.permutation(single, ROWS_DEV * N_ROW)[:K]).astype(jnp.int32)
    return jax.vmap(pick)(keys)


def shard_levels(own_key, extent, shards, least, top_value):
    loudness, own = 1.0, jax.random.fold_in(own_key, 6)
    for dim, shards_of in shards:
        heights = jnp.exp(jax.random.uniform(jax.random.fold_in(own, dim), (shards_of,), jnp.float32, least / len(shards), top_value / len(shards)))
        loudness = loudness * jnp.repeat(heights, extent[dim] // shards_of).reshape([-1 if axis == dim else 1 for axis in range(len(extent))])
    return loudness


def centred(rng, extent, deviation, reach, cuts=(), held_as=jnp.bfloat16):
    factor_of = shard_levels(rng, extent, cuts, -0.22, 0.18) if cuts else 1.0
    entries = jax.random.normal(rng, extent, jnp.float32) * deviation * factor_of
    return jnp.minimum(jnp.maximum(entries, -reach), reach).astype(held_as)


def setup_inputs(seed: int = 0, part: int = 0) -> dict:
    arg_keys = jax.random.split(jax.random.key(seed), 4)
    part_keys = jax.random.split(jax.random.fold_in(arg_keys[3], part), 4)
    samples = centred(part_keys[0], (FRONTS, ROWS, C), 1.0, 6.0, ((1, 16),))
    column_order = jax.vmap(lambda own: jax.random.permutation(own, C))(jax.random.split(part_keys[1], FRONTS)).reshape((FRONTS, C)).astype(jnp.int32)
    skeleton = draw_skeleton(jax.random.fold_in(jax.random.fold_in(arg_keys[3], part), 71), part)
    return {"samples": samples, "column_order": column_order, "skeleton": skeleton}


def one_front(block, order, skel):
    permuted = block[:, order].astype(jnp.float32)
    gram = jnp.dot(permuted.T, permuted, precision=lax.Precision.HIGHEST) / ROWS
    lower = jnp.linalg.cholesky(gram)
    q_factor = jax.scipy.linalg.solve_triangular(lower, permuted.T, lower=True).T
    qskel = q_factor[skel.astype(jnp.int32)]
    small = jnp.dot(qskel, qskel.T, precision=lax.Precision.HIGHEST)
    lower_small = jnp.linalg.cholesky(small)
    cross = jnp.dot(q_factor, qskel.T, precision=lax.Precision.HIGHEST)
    inner = jax.scipy.linalg.solve_triangular(lower_small, cross.T, lower=True)
    interp = jax.scipy.linalg.solve_triangular(lower_small, inner, lower=True, trans='T').T
    return (q_factor, interp.astype(jnp.bfloat16))

def reference(samples, column_order, skeleton):
    q_factor, interp = jax.vmap(one_front)(samples, column_order, skeleton)
    return (q_factor, interp)
```

```python
import functools

import jax
import jax.numpy as jnp
from jax import lax
from jax.experimental import pallas as pl
from jax.experimental.pallas import tpu as pltpu
from jax.sharding import PartitionSpec as P

F32, BF16 = jnp.float32, jnp.bfloat16
BLOCK = 128
PANEL = 8
VMEM = pltpu.VMEM


def split(x):
    high = x.astype(BF16).astype(F32)
    rest = x - high
    mid = rest.astype(BF16).astype(F32)
    return high, mid, rest - mid


def pair(x):
    high = x.astype(BF16)
    return high, (x - high.astype(F32)).astype(BF16)


def mul(a, b, dims, exact=True):
    return lax.dot_general(
        a, b, (dims, ((), ())),
        precision=lax.Precision.HIGHEST if exact else None,
        preferred_element_type=F32,
    )


NN, NT, TN = ((1,), (0,)), ((1,), (1,)), ((0,), (0,))


def row(x, k):
    return jnp.broadcast_to(x[k:k + 1], x.shape)


def take(x, index):
    return jnp.take_along_axis(x, index, axis=1)


def identity():
    r = lax.broadcasted_iota(jnp.int32, (BLOCK, BLOCK), 0)
    c = lax.broadcasted_iota(jnp.int32, (BLOCK, BLOCK), 1)
    return jnp.where(r == c, 1.0, 0.0).astype(F32)


def invert_block(work, inverse):
    sub = lax.broadcasted_iota(jnp.int32, (PANEL, BLOCK), 0)
    lane = lax.broadcasted_iota(jnp.int32, (PANEL, BLOCK), 1)

    def panel(p, carry):
        here_a, here_e, last_a, last_e = carry
        base = pl.multiple_of(PANEL * p, PANEL)
        at = sub + base
        after = (at + PANEL) & (BLOCK - 1)
        left = split(jnp.where(lane >= base + 2 * PANEL, last_a, 0.0))
        right = split(jnp.concatenate([last_a, last_e], axis=1))
        lhs = jnp.concatenate([left[i] for i in (0, 0, 1, 0, 1, 2)], axis=0).astype(BF16)
        rhs = jnp.concatenate([right[i] for i in (0, 1, 0, 2, 1, 0)], axis=0).astype(BF16)
        next_a = work[pl.ds(base + PANEL, PANEL), :BLOCK]
        next_e = work[pl.ds(base + PANEL, PANEL), BLOCK:]
        work[:BLOCK, :] = work[:BLOCK, :] - mul(lhs, rhs, TN, exact=False)
        for k in range(PANEL):
            coef = take(row(last_a, k), after)
            next_a = next_a - coef * row(last_a, k)
            next_e = next_e - coef * row(last_e, k)
        own = [take(row(here_a, k), at) for k in range(PANEL)]
        down = [take(row(here_a, k), after) for k in range(PANEL)]
        for k in range(PANEL):
            scale = lax.rsqrt(row(own[k], k))
            lo, ln = own[k] * scale, down[k] * scale
            for m in range(k + 1, PANEL):
                s = row(lo, m)
                own[m] = own[m] - lo * s
                down[m] = down[m] - ln * s
            ua, ue = row(here_a, k) * scale, row(here_e, k) * scale
            below = jnp.where(sub > k, lo, 0.0)
            here_a = jnp.where(sub == k, ua, here_a - below * ua)
            here_e = jnp.where(sub == k, ue, here_e - below * ue)
            next_a = next_a - ln * ua
            next_e = next_e - ln * ue
        inverse[pl.ds(base, PANEL), :] = here_e
        return next_a, next_e, here_a, here_e

    zero = jnp.zeros((PANEL, BLOCK), F32)
    first = (work[:PANEL, :BLOCK], work[:PANEL, BLOCK:], zero, zero)
    lax.fori_loop(0, BLOCK // PANEL, panel, first, unroll=4)


def eliminate(both, n, work, inverse):
    half = n * BLOCK
    work[BLOCK:, :] = jnp.zeros((PANEL, 2 * BLOCK), F32)
    for j in range(n):
        rows = pl.ds(j * BLOCK, BLOCK)
        work[:BLOCK, :BLOCK] = both[rows, j * BLOCK:(j + 1) * BLOCK]
        work[:BLOCK, BLOCK:] = identity()
        invert_block(work, inverse)
        w = inverse[...]
        first, end = (j + 1) * BLOCK, half + j * BLOCK
        both[rows, first:end] = mul(w, both[rows, first:end], NN)
        both[rows, end:end + BLOCK] = w
        for i in range(j + 1, n):
            lead = both[rows, i * BLOCK:(i + 1) * BLOCK]
            below = pl.ds(i * BLOCK, BLOCK)
            span = slice(i * BLOCK, end + BLOCK)
            both[below, span] = both[below, span] - mul(lead, both[rows, span], TN)


def finish(rows_total, sums_ref, xp_ref, q_ref, interp_ref, big, little, work, inverse):
    cols = xp_ref.shape[1]
    n, m = cols // BLOCK, (sums_ref.shape[1] // PANEL - 6) // (cols // BLOCK)
    grab = lambda b: sums_ref[:, b * PANEL:(b + 1) * PANEL, :].reshape(BLOCK, BLOCK)
    big[...] = jnp.zeros_like(big)
    b = 0
    for i in range(n):
        for j in range(i, n):
            big[i * BLOCK:(i + 1) * BLOCK, j * BLOCK:(j + 1) * BLOCK] = grab(b) * (1.0 / rows_total)
            b += 1
    eliminate(big, n, work, inverse)
    e = big[:, cols:]
    yskel = jnp.concatenate(
        [jnp.concatenate([grab(b + i * n + j) for j in range(n)], axis=1) for i in range(m)], axis=0
    )
    qskel = mul(yskel, e, NT)
    little[:, m * BLOCK:] = jnp.zeros((m * BLOCK, m * BLOCK), F32)
    little[:, :m * BLOCK] = mul(qskel, qskel, NT)
    eliminate(little, m, work, inverse)
    w = little[:, m * BLOCK:]
    right = mul(w, mul(w, qskel, NN), TN)
    e_high, e_low = pair(e)
    r_high, r_low = pair(right)

    @pl.loop(0, xp_ref.shape[0] // 256)
    def _(step):
        rows = pl.ds(pl.multiple_of(step * 256, 256), 256)
        x = xp_ref[rows, :]
        q = mul(x, e_high, NT, False) + mul(x, e_low, NT, False)
        q_ref[rows, :] = q
        q_high, q_low = pair(q)
        out = mul(q_high, r_high, NT, False) + mul(q_low, r_high, NT, False) + mul(q_high, r_low, NT, False)
        interp_ref[rows, :] = out.astype(BF16)


def exchange(count, samples_ref, order_ref, skel_ref, sums_ref, xp_ref,
             mine, inbox, total, out_sem, in_sem, out_sem2, in_sem2):
    me = lax.axis_index("row")
    rows, cols = samples_ref.shape
    barrier = pltpu.get_barrier_semaphore()
    for s in range(1, count):
        pl.semaphore_signal(
            barrier, inc=1, device_id={"row": lax.rem(me + s, count)}, device_id_type=pl.DeviceIdType.MESH)
    place = lax.broadcasted_iota(jnp.int32, (cols, cols), 0)
    move = jnp.where(place == order_ref[...], 1.0, 0.0).astype(BF16)
    xp_ref[...] = mul(samples_ref[...], move, NN, False).astype(BF16)
    keys = skel_ref.shape[1]
    at = lax.broadcasted_iota(jnp.int32, (rows, keys), 0) + me * rows
    pick = jnp.where(at == skel_ref[...], 1.0, 0.0).astype(BF16)
    xp = xp_ref[...]
    n = cols // BLOCK

    def put(b, value):
        mine[:, b * PANEL:(b + 1) * PANEL, :] = value.reshape(count, PANEL, BLOCK)

    b = 0
    for i in range(n):
        part = mul(xp[:, i * BLOCK:(i + 1) * BLOCK], xp[:, i * BLOCK:], TN, False)
        for j in range(i, n):
            put(b, part[:, (j - i) * BLOCK:(j - i + 1) * BLOCK])
            b += 1
    chosen = mul(pick, xp, TN, False)
    for i in range(keys // BLOCK):
        for j in range(n):
            put(b, chosen[i * BLOCK:(i + 1) * BLOCK, j * BLOCK:(j + 1) * BLOCK])
            b += 1
    pl.semaphore_wait(barrier, count - 1)
    steps = sorted(range(1, count), key=lambda s: -min(s, count - s))

    def send(source, target, s, a, b):
        return pltpu.make_async_remote_copy(
            src_ref=source, dst_ref=target, send_sem=a.at[s], recv_sem=b.at[s],
            device_id={"row": lax.rem(me + s, count)}, device_id_type=pl.DeviceIdType.MESH)

    scatter = {s: send(mine.at[lax.rem(me + s, count)], inbox.at[s], s, out_sem, in_sem) for s in steps}
    for s in steps:
        scatter[s].start()
    acc = mine[me]
    for s in reversed(steps):
        scatter[s].wait_recv()
        acc = acc + inbox[s]
    total[me] = acc
    gather = {s: send(total.at[me], total.at[me], s, out_sem2, in_sem2) for s in steps}
    for s in steps:
        gather[s].start()
    for s in steps:
        scatter[s].wait_send()
    for s in reversed(steps):
        gather[s].wait_send()
        gather[s].wait_recv()
    sums_ref[...] = total[...]


def on_device(count, samples, column_order, skeleton):
    _, rows, cols = samples.shape
    keys = skeleton.shape[1]
    n, m = cols // BLOCK, keys // BLOCK
    depth = (n * (n + 1) // 2 + m * n) * PANEL
    whole = pl.BlockSpec(memory_space=VMEM)
    sums, permuted = pl.pallas_call(
        functools.partial(exchange, count),
        out_shape=(jax.ShapeDtypeStruct((count, depth, BLOCK), F32), jax.ShapeDtypeStruct((rows, cols), BF16)),
        in_specs=[whole] * 3,
        out_specs=(whole, whole),
        scratch_shapes=[VMEM((count, depth, BLOCK), F32)] * 3 + [pltpu.SemaphoreType.DMA((count,))] * 4,
        compiler_params=pltpu.CompilerParams(collective_id=0, has_side_effects=True),
    )(samples[0], column_order, skeleton)
    q_factor, interp = pl.pallas_call(
        functools.partial(finish, rows * count),
        out_shape=(jax.ShapeDtypeStruct((rows, cols), F32), jax.ShapeDtypeStruct((rows, keys), BF16)),
        in_specs=[whole] * 2,
        out_specs=(whole, whole),
        scratch_shapes=[
            VMEM((cols, 2 * cols), F32), VMEM((keys, 2 * keys), F32),
            VMEM((BLOCK + PANEL, 2 * BLOCK), F32), VMEM((BLOCK, BLOCK), F32),
        ],
    )(sums, permuted)
    return q_factor[None], interp[None]


def solution(mesh):
    placed = (P("node", "row", None), P("node", None), P("node", None))
    return jax.shard_map(
        functools.partial(on_device, mesh.shape["row"]),
        mesh=mesh,
        in_specs=placed,
        out_specs=(P("node", "row", None), P("node", "row", None)),
        check_vma=False,
    )
```

```python
import jax
import jax.numpy as jnp
from jax import lax
from jax.experimental import pallas as pl
from jax.experimental.pallas import tpu as pltpu
from jax.sharding import PartitionSpec as P

F32, BF16 = jnp.float32, jnp.bfloat16
BLOCK = 128
PANEL = 8
RING = 16
VMEM = pltpu.VMEM


def split(x):
    high = x.astype(BF16).astype(F32)
    rest = x - high
    mid = rest.astype(BF16).astype(F32)
    return high, mid, rest - mid


def pair(x):
    high = x.astype(BF16)
    return high, (x - high.astype(F32)).astype(BF16)


def mul(a, b, dims, exact=True):
    return lax.dot_general(
        a, b, (dims, ((), ())),
        precision=lax.Precision.HIGHEST if exact else None,
        preferred_element_type=F32,
    )


NN, NT, TN = ((1,), (0,)), ((1,), (1,)), ((0,), (0,))


def row(x, k):
    return jnp.broadcast_to(x[k:k + 1], x.shape)


def take(x, index):
    return jnp.take_along_axis(x, index, axis=1)


def identity():
    r = lax.broadcasted_iota(jnp.int32, (BLOCK, BLOCK), 0)
    c = lax.broadcasted_iota(jnp.int32, (BLOCK, BLOCK), 1)
    return jnp.where(r == c, 1.0, 0.0).astype(F32)


def invert_block(work, inverse):
    sub = lax.broadcasted_iota(jnp.int32, (PANEL, BLOCK), 0)
    lane = lax.broadcasted_iota(jnp.int32, (PANEL, BLOCK), 1)

    def panel(p, carry):
        here_a, here_e, last_a, last_e = carry
        base = pl.multiple_of(PANEL * p, PANEL)
        at = sub + base
        after = (at + PANEL) & (BLOCK - 1)
        left = split(jnp.where(lane >= base + 2 * PANEL, last_a, 0.0))
        right = split(jnp.concatenate([last_a, last_e], axis=1))
        lhs = jnp.concatenate([left[i] for i in (0, 0, 1, 0, 1, 2)], axis=0).astype(BF16)
        rhs = jnp.concatenate([right[i] for i in (0, 1, 0, 2, 1, 0)], axis=0).astype(BF16)
        next_a = work[pl.ds(base + PANEL, PANEL), :BLOCK]
        next_e = work[pl.ds(base + PANEL, PANEL), BLOCK:]
        work[:BLOCK, :] = work[:BLOCK, :] - mul(lhs, rhs, TN, exact=False)
        for k in range(PANEL):
            coef = take(row(last_a, k), after)
            next_a = next_a - coef * row(last_a, k)
            next_e = next_e - coef * row(last_e, k)
        own = [take(row(here_a, k), at) for k in range(PANEL)]
        down = [take(row(here_a, k), after) for k in range(PANEL)]
        for k in range(PANEL):
            scale = lax.rsqrt(row(own[k], k))
            lo, ln = own[k] * scale, down[k] * scale
            for m in range(k + 1, PANEL):
                s = row(lo, m)
                own[m] = own[m] - lo * s
                down[m] = down[m] - ln * s
            ua, ue = row(here_a, k) * scale, row(here_e, k) * scale
            below = jnp.where(sub > k, lo, 0.0)
            here_a = jnp.where(sub == k, ua, here_a - below * ua)
            here_e = jnp.where(sub == k, ue, here_e - below * ue)
            next_a = next_a - ln * ua
            next_e = next_e - ln * ue
        inverse[pl.ds(base, PANEL), :] = here_e
        return next_a, next_e, here_a, here_e

    zero = jnp.zeros((PANEL, BLOCK), F32)
    first = (work[:PANEL, :BLOCK], work[:PANEL, BLOCK:], zero, zero)
    lax.fori_loop(0, BLOCK // PANEL, panel, first, unroll=4)


def eliminate(both, n, work, inverse, between=None):
    half = n * BLOCK
    work[BLOCK:, :] = jnp.zeros((PANEL, 2 * BLOCK), F32)
    for j in range(n):
        rows = pl.ds(j * BLOCK, BLOCK)
        work[:BLOCK, :BLOCK] = both[rows, j * BLOCK:(j + 1) * BLOCK]
        work[:BLOCK, BLOCK:] = identity()
        invert_block(work, inverse)
        if between is not None and j == 0:
            between()
        w = inverse[...]
        first, end = (j + 1) * BLOCK, half + j * BLOCK
        both[rows, first:end] = mul(w, both[rows, first:end], NN)
        both[rows, end:end + BLOCK] = w
        for i in range(j + 1, n):
            lead = both[rows, i * BLOCK:(i + 1) * BLOCK]
            below = pl.ds(i * BLOCK, BLOCK)
            span = slice(i * BLOCK, end + BLOCK)
            both[below, span] = both[below, span] - mul(lead, both[rows, span], TN)


def finish(e_ref, yskel_ref, xp_ref, q_ref, interp_ref, little, work, inverse):
    keys = yskel_ref.shape[0]
    e = e_ref[...]
    qskel = mul(yskel_ref[...], e, NT)
    little[:, keys:] = jnp.zeros((keys, keys), F32)
    little[:, :keys] = mul(qskel, qskel, NT)
    eliminate(little, keys // BLOCK, work, inverse)
    w = little[:, keys:]
    right = mul(w, mul(w, qskel, NN), TN)
    e_high, e_low = pair(e)
    r_high, r_low = pair(right)

    @pl.loop(0, xp_ref.shape[0] // 256)
    def _(step):
        rows = pl.ds(pl.multiple_of(step * 256, 256), 256)
        x = xp_ref[rows, :]
        q = mul(x, e_high, NT, False) + mul(x, e_low, NT, False)
        q_ref[rows, :] = q
        q_high, q_low = pair(q)
        out = mul(q_high, r_high, NT, False) + mul(q_low, r_high, NT, False) + mul(q_high, r_low, NT, False)
        interp_ref[rows, :] = out.astype(BF16)


def places():
    r = lax.broadcasted_iota(jnp.int32, (BLOCK, BLOCK), 0)
    c = lax.broadcasted_iota(jnp.int32, (BLOCK, BLOCK), 1)
    return r, c


def fold(first, second, third):
    r, c = places()
    edge = jnp.sum(jnp.where(r == c, first, 0.0), axis=0, keepdims=True)
    corner = first[BLOCK - 1:, BLOCK - 1:]
    one = jnp.where(r > c, first, second)
    two = jnp.where(r == c + 1, edge, third)
    return one, jnp.where((r == BLOCK - 1) & (c == 0), corner, two)


def unfold(one, two):
    r, c = places()
    edge = jnp.sum(jnp.where(r == c + 1, two, 0.0), axis=0, keepdims=True)
    corner = two[BLOCK - 1:, :1]
    edge = jnp.where(c == BLOCK - 1, corner, edge)
    first = jnp.where(r < c, one.T, jnp.where(r == c, edge, 0.0))
    return first, jnp.where(r <= c, one, 0.0), jnp.where(r <= c, two, 0.0)


def exchange(samples_ref, order_ref, skel_ref, e_ref, yskel_ref, xp_ref,
             gmine, gnear, gedge, gpart, gmate, gfull,
             ymine, ynear, yedge, ypart, ymate, yfull,
             big, work, inverse, out_sem, in_sem):
    me = lax.axis_index("row")
    rows, cols = samples_ref.shape
    keys = skel_ref.shape[1]
    n, m = cols // BLOCK, keys // BLOCK
    around = lambda d, size: lax.rem(me + (d + RING), size)
    barrier = pltpu.get_barrier_semaphore()
    near = (3, -3, 2, -2, 1, -1)
    partners = (8, 4, -4) + near
    for d in partners:
        pl.semaphore_signal(
            barrier, inc=1, device_id={"row": around(d, RING)}, device_id_type=pl.DeviceIdType.MESH)
    number = iter(range(32))

    def send(source, target, d):
        i = next(number)
        copy = pltpu.make_async_remote_copy(
            src_ref=source, dst_ref=target, send_sem=out_sem.at[i], recv_sem=in_sem.at[i],
            device_id={"row": around(d, RING)}, device_id_type=pl.DeviceIdType.MESH)
        copy.start()
        return copy

    place = lax.broadcasted_iota(jnp.int32, (cols, cols), 0)
    move = jnp.where(place == order_ref[...], 1.0, 0.0).astype(BF16)
    xp_ref[...] = mul(samples_ref[...], move, NN, False).astype(BF16)
    xp = xp_ref[...]
    parts = [
        [mul(xp[:, i * BLOCK:(i + 1) * BLOCK], xp[:, i * BLOCK:], TN, False)[:, j * BLOCK:(j + 1) * BLOCK]
         for j in range(n - i)] for i in range(n)
    ]
    folded = fold(*[parts[i][0] for i in range(n)]) + (parts[0][1], parts[0][2], parts[1][1])
    for b, value in enumerate(folded):
        gmine[:, b * 16:(b + 1) * 16, :] = value.reshape(8, 16, BLOCK)
    pl.semaphore_wait(barrier, len(partners))

    sent = []
    unit = around(0, 8)
    ghalf = gmine.shape[1] // 2
    ends = ((4, 0), (-4, 1))
    here = [send(gmine.at[around(4, 8), pl.ds(h * ghalf, ghalf)], gedge.at[h], d) for d, h in ends]
    here += [send(gmine.at[around(d, 8)], gnear.at[k], d) for k, d in enumerate(near)]
    sent += here

    at = lax.broadcasted_iota(jnp.int32, (rows, keys), 0) + me * rows
    pick = jnp.where(at == skel_ref[...], 1.0, 0.0).astype(BF16)
    chosen = mul(pick, xp, TN, False)
    for b in range(m * n):
        i, j = b // n, b % n
        value = chosen[i * BLOCK:(i + 1) * BLOCK, j * BLOCK:(j + 1) * BLOCK].reshape(4, 4, PANEL, BLOCK)
        for k in range(4):
            ymine[k, :, b * PANEL:(b + 1) * PANEL, :] = value[:, k]
    residue, quarter = around(0, 4), lax.div(me, 4)
    yhalf = ymine.shape[2] // 2
    pairs = ((2, 0), (-2, 1))
    there = [send(ymine.at[around(2, 4), :, pl.ds(h * yhalf, yhalf)], yedge.at[h], d) for d, h in pairs]
    there += [send(ymine.at[around(d, 4)], ynear.at[k], d) for k, d in enumerate((1, -1))]
    sent += there

    for copy in here:
        copy.wait_recv()
    acc = gmine[unit] + jnp.concatenate([gedge[0], gedge[1]], axis=0)
    for k in range(len(near)):
        acc = acc + gnear[k]
    gpart[...] = acc
    across = send(gpart, gmate, 8)
    sent.append(across)

    for copy in there:
        copy.wait_recv()
    ypart[...] = ymine[residue] + ynear[0] + ynear[1] + jnp.concatenate([yedge[0], yedge[1]], axis=1)
    far = (8, 4, -4)
    there = [send(ypart.at[lax.rem(quarter + (d // 4 + 4), 4)], ymate.at[k], d) for k, d in enumerate(far)]
    sent += there

    across.wait_recv()
    gfull[unit] = gpart[...] + gmate[...]
    here = []
    for d, h in ends:
        piece = gfull.at[unit, pl.ds(h * ghalf, ghalf)]
        here.append(send(piece, piece, d))
    here += [send(gfull.at[unit], gfull.at[unit], d) for d in near]
    sent += here

    for copy in there:
        copy.wait_recv()
    yfull[residue, quarter] = ypart[quarter] + ymate[0] + ymate[1] + ymate[2]
    there = [send(yfull.at[residue, quarter], yfull.at[residue, quarter], d) for d in far]
    sent += there

    for copy in here:
        copy.wait_recv()
    scale = 1.0 / (rows * RING)
    full = [gfull[:, b * 16:(b + 1) * 16, :].reshape(BLOCK, BLOCK) * scale for b in range(len(folded))]
    big[...] = jnp.zeros_like(big)
    for i, value in enumerate(unfold(full[0], full[1])):
        big[i * BLOCK:(i + 1) * BLOCK, i * BLOCK:(i + 1) * BLOCK] = value
    for (i, j), value in zip(((0, 1), (0, 2), (1, 2)), full[2:]):
        big[i * BLOCK:(i + 1) * BLOCK, j * BLOCK:(j + 1) * BLOCK] = value

    last = []

    def hand_on():
        for copy in there:
            copy.wait_recv()
        for d, h in pairs:
            piece = yfull.at[residue, :, pl.ds(h * yhalf, yhalf)]
            last.append(send(piece, piece, d))
        for d in (1, -1):
            last.append(send(yfull.at[residue], yfull.at[residue], d))

    eliminate(big, n, work, inverse, hand_on)
    e_ref[...] = big[:, cols:]
    for copy in last:
        copy.wait_recv()
    for b in range(m * n):
        i, j = b // n, b % n
        value = jnp.stack([yfull[k, :, b * PANEL:(b + 1) * PANEL, :] for k in range(4)], axis=1)
        yskel_ref[i * BLOCK:(i + 1) * BLOCK, j * BLOCK:(j + 1) * BLOCK] = value.reshape(BLOCK, BLOCK)
    for copy in sent + last:
        copy.wait_send()


def on_device(samples, column_order, skeleton):
    _, rows, cols = samples.shape
    keys = skeleton.shape[1]
    n, m = cols // BLOCK, keys // BLOCK
    whole = pl.BlockSpec(memory_space=VMEM)
    deep, tall = 5 * 16, m * n * PANEL
    room = [VMEM((BLOCK + PANEL, 2 * BLOCK), F32), VMEM((BLOCK, BLOCK), F32)]
    e, yskel, permuted = pl.pallas_call(
        exchange,
        out_shape=(
            jax.ShapeDtypeStruct((cols, cols), F32), jax.ShapeDtypeStruct((keys, cols), F32),
            jax.ShapeDtypeStruct((rows, cols), BF16),
        ),
        in_specs=[whole] * 3,
        out_specs=(whole,) * 3,
        scratch_shapes=[
            VMEM((8, deep, BLOCK), F32), VMEM((6, deep, BLOCK), F32), VMEM((2, deep // 2, BLOCK), F32),
            VMEM((deep, BLOCK), F32), VMEM((deep, BLOCK), F32), VMEM((8, deep, BLOCK), F32),
            VMEM((4, 4, tall, BLOCK), F32), VMEM((2, 4, tall, BLOCK), F32), VMEM((2, 4, tall // 2, BLOCK), F32),
            VMEM((4, tall, BLOCK), F32), VMEM((3, tall, BLOCK), F32), VMEM((4, 4, tall, BLOCK), F32),
            VMEM((cols, 2 * cols), F32),
        ] + room + [pltpu.SemaphoreType.DMA((32,))] * 2,
        compiler_params=pltpu.CompilerParams(collective_id=0, has_side_effects=True),
    )(samples[0], column_order, skeleton)
    q_factor, interp = pl.pallas_call(
        finish,
        out_shape=(jax.ShapeDtypeStruct((rows, cols), F32), jax.ShapeDtypeStruct((rows, keys), BF16)),
        in_specs=[whole] * 3,
        out_specs=(whole, whole),
        scratch_shapes=[VMEM((keys, 2 * keys), F32)] + room,
    )(e, yskel, permuted)
    return q_factor[None], interp[None]


def solution(mesh):
    placed = (P("node", "row", None), P("node", None), P("node", None))
    return jax.shard_map(
        on_device,
        mesh=mesh,
        in_specs=placed,
        out_specs=(P("node", "row", None), P("node", "row", None)),
        check_vma=False,
    )
```

```python
import functools

import jax
import jax.numpy as jnp
from jax import lax
from jax.experimental import pallas as pl
from jax.experimental.pallas import tpu as pltpu
from jax.sharding import PartitionSpec as P

F32, BF16 = jnp.float32, jnp.bfloat16
BLOCK = 128
PANEL = 8
RING = 16
VMEM = pltpu.VMEM


def split(x):
    high = x.astype(BF16).astype(F32)
    rest = x - high
    mid = rest.astype(BF16).astype(F32)
    return high, mid, rest - mid


def pair(x):
    high = x.astype(BF16)
    return high, (x - high.astype(F32)).astype(BF16)


def mul(a, b, dims, exact=True):
    return lax.dot_general(
        a, b, (dims, ((), ())),
        precision=lax.Precision.HIGHEST if exact else None,
        preferred_element_type=F32,
    )


NN, NT, TN = ((1,), (0,)), ((1,), (1,)), ((0,), (0,))


def row(x, k):
    return jnp.broadcast_to(x[k:k + 1], x.shape)


def take(x, index):
    return jnp.take_along_axis(x, index, axis=1)


def identity():
    r = lax.broadcasted_iota(jnp.int32, (BLOCK, BLOCK), 0)
    c = lax.broadcasted_iota(jnp.int32, (BLOCK, BLOCK), 1)
    return jnp.where(r == c, 1.0, 0.0).astype(F32)


def invert_block(work, inverse, beside=None):
    sub = lax.broadcasted_iota(jnp.int32, (PANEL, BLOCK), 0)
    lane = lax.broadcasted_iota(jnp.int32, (PANEL, BLOCK), 1)

    def panel(p, carry):
        here_a, here_e, last_a, last_e = carry
        base = pl.multiple_of(PANEL * p, PANEL)
        at = sub + base
        after = (at + PANEL) & (BLOCK - 1)
        left = split(jnp.where(lane >= base + 2 * PANEL, last_a, 0.0))
        right = split(jnp.concatenate([last_a, last_e], axis=1))
        lhs = jnp.concatenate([left[i] for i in (0, 0, 1, 0, 1, 2)], axis=0).astype(BF16)
        rhs = jnp.concatenate([right[i] for i in (0, 1, 0, 2, 1, 0)], axis=0).astype(BF16)
        next_a = work[pl.ds(base + PANEL, PANEL), :BLOCK]
        next_e = work[pl.ds(base + PANEL, PANEL), BLOCK:]
        work[:BLOCK, :] = work[:BLOCK, :] - mul(lhs, rhs, TN, exact=False)
        for k in range(PANEL):
            coef = take(row(last_a, k), after)
            next_a = next_a - coef * row(last_a, k)
            next_e = next_e - coef * row(last_e, k)
        own = [take(row(here_a, k), at) for k in range(PANEL)]
        down = [take(row(here_a, k), after) for k in range(PANEL)]
        for k in range(PANEL):
            scale = lax.rsqrt(row(own[k], k))
            lo, ln = own[k] * scale, down[k] * scale
            for m in range(k + 1, PANEL):
                s = row(lo, m)
                own[m] = own[m] - lo * s
                down[m] = down[m] - ln * s
            ua, ue = row(here_a, k) * scale, row(here_e, k) * scale
            below = jnp.where(sub > k, lo, 0.0)
            here_a = jnp.where(sub == k, ua, here_a - below * ua)
            here_e = jnp.where(sub == k, ue, here_e - below * ue)
            next_a = next_a - ln * ua
            next_e = next_e - ln * ue
        inverse[pl.ds(base, PANEL), :] = here_e
        return next_a, next_e, here_a, here_e

    def several(step, carry):
        if beside is not None:
            beside(step)
        for k in range(4):
            carry = panel(step * 4 + k, carry)
        return carry

    zero = jnp.zeros((PANEL, BLOCK), F32)
    first = (work[:PANEL, :BLOCK], work[:PANEL, BLOCK:], zero, zero)
    lax.fori_loop(0, BLOCK // PANEL // 4, several, first)


def eliminate(both, n, work, inverse, right=None, between=None, beside=None):
    half = n * BLOCK
    work[BLOCK:, :] = jnp.zeros((PANEL, 2 * BLOCK), F32)
    for j in range(n):
        rows = pl.ds(j * BLOCK, BLOCK)
        work[:BLOCK, :BLOCK] = both[rows, j * BLOCK:(j + 1) * BLOCK]
        work[:BLOCK, BLOCK:] = identity()
        invert_block(work, inverse, functools.partial(beside, j) if beside is not None else None)
        if between is not None:
            between(j)
        w = inverse[...]
        first, end = (j + 1) * BLOCK, half + j * BLOCK
        both[rows, first:end] = mul(w, both[rows, first:end], NN)
        both[rows, end:end + BLOCK] = w
        if right is not None:
            right[rows, :] = mul(w, right[rows, :], NN)
        for i in range(j + 1, n):
            lead = both[rows, i * BLOCK:(i + 1) * BLOCK]
            below = pl.ds(i * BLOCK, BLOCK)
            span = slice(i * BLOCK, end + BLOCK)
            both[below, span] = both[below, span] - mul(lead, both[rows, span], TN)
            if right is not None:
                right[below, :] = right[below, :] - mul(lead, right[rows, :], TN)


def finish(q_ref, high_ref, low_ref, right_ref, q_out, interp_out, interp, sems):
    whole_q = pltpu.make_async_copy(q_ref, q_out, sems.at[0])
    whole_q.start()
    r_high, r_low = pair(right_ref[...])
    size = q_ref.shape[0] // 4
    copies = []
    for step in range(4):
        rows = pl.ds(step * size, size)
        high, low = high_ref[rows, :], low_ref[rows, :]
        out = mul(high, r_high, NT, False) + mul(low, r_high, NT, False) + mul(high, r_low, NT, False)
        interp[rows, :] = out.astype(BF16)
        copies.append(pltpu.make_async_copy(interp.at[rows, :], interp_out.at[rows, :], sems.at[1 + step]))
        copies[-1].start()
    whole_q.wait()
    for copy in copies:
        copy.wait()


def places():
    r = lax.broadcasted_iota(jnp.int32, (BLOCK, BLOCK), 0)
    c = lax.broadcasted_iota(jnp.int32, (BLOCK, BLOCK), 1)
    return r, c


def fold(first, second, third):
    r, c = places()
    edge = jnp.sum(jnp.where(r == c, first, 0.0), axis=0, keepdims=True)
    corner = first[BLOCK - 1:, BLOCK - 1:]
    one = jnp.where(r > c, first, second)
    two = jnp.where(r == c + 1, edge, third)
    return one, jnp.where((r == BLOCK - 1) & (c == 0), corner, two)


def unfold(one, two):
    r, c = places()
    edge = jnp.sum(jnp.where(r == c + 1, two, 0.0), axis=0, keepdims=True)
    corner = two[BLOCK - 1:, :1]
    edge = jnp.where(c == BLOCK - 1, corner, edge)
    first = jnp.where(r < c, one.T, jnp.where(r == c, edge, 0.0))
    return first, jnp.where(r <= c, one, 0.0), jnp.where(r <= c, two, 0.0)


class Stream:
    def __init__(self, me, send, mine, near, edge, part, mate, full):
        self.me, self.send = me, send
        self.mine, self.near, self.edge = mine, near, edge
        self.part, self.mate, self.full = part, mate, full
        self.residue, self.quarter = lax.rem(me, 4), lax.div(me, 4)
        self.sent, self.due = [], []

    def begin(self, copies):
        self.due = copies
        self.sent += copies

    def arrive(self):
        for copy in self.due:
            copy.wait_recv()

    def put(self, b, value):
        value = value.reshape(4, 4, PANEL, BLOCK)
        for k in range(4):
            self.mine[k, :, b * PANEL:(b + 1) * PANEL, :] = value[:, k]

    def get(self, b):
        value = jnp.stack([self.full[k, :, b * PANEL:(b + 1) * PANEL, :] for k in range(4)], axis=1)
        return value.reshape(BLOCK, BLOCK)

    def spread(self):
        self.begin(
            [self.send(self.mine.at[lax.rem(self.me + 2, 4), pl.ds(h, 2)], self.edge.at[pl.ds(h, 2)], d)
             for d, h in ((2, 0), (-2, 2))]
            + [self.send(self.mine.at[lax.rem(self.me + d + RING, 4)], self.near.at[k], d)
               for k, d in enumerate((1, -1))])

    def reduce_near(self):
        self.arrive()
        self.part[...] = (self.mine[self.residue] + self.edge[...]) + (self.near[0] + self.near[1])
        self.begin([self.send(self.part.at[lax.rem(self.quarter + (d // 4 + 4), 4)], self.mate.at[k], d)
                    for k, d in enumerate((8, 4, -4))])

    def reduce_far(self):
        self.arrive()
        own = self.full.at[self.residue, self.quarter]
        own[...] = (self.part[self.quarter] + self.mate[0]) + (self.mate[1] + self.mate[2])
        self.begin([self.send(own, own, d) for d in (8, 4, -4)])

    def hand_back(self):
        self.arrive()
        piece = lambda h: self.full.at[self.residue, pl.ds(h, 2)]
        self.begin([self.send(piece(h), piece(h), d) for d, h in ((2, 0), (-2, 2))]
                   + [self.send(self.full.at[self.residue], self.full.at[self.residue], d) for d in (1, -1)])

    def drain(self):
        for copy in self.sent:
            copy.wait_send()


def room_of(blocks):
    rows = blocks * PANEL
    return [VMEM(shape + (rows, BLOCK), F32) for shape in ((4, 4), (2, 4), (4,), (4,), (3,), (4, 4))]


def factor(samples_hbm, order_hbm, skel_hbm, q_ref, high_ref, low_ref, right_ref, *scratch):
    streams = scratch[:24]
    (big, little, solved, samples, xp_ref, order_ref, skel_ref, work, inverse, out_sem, in_sem, load_sem, known) = scratch[24:]
    me = lax.axis_index("row")
    rows, cols = samples.shape
    keys = skel_ref.shape[1]
    n, m = cols // BLOCK, keys // BLOCK
    around = lambda d: lax.rem(me + (d + RING), RING)
    barrier = pltpu.get_barrier_semaphore()
    partners = (2, -2, 1, -1)
    for d in partners:
        pl.semaphore_signal(
            barrier, inc=1, device_id={"row": around(d)}, device_id_type=pl.DeviceIdType.MESH)
    loads = [pltpu.make_async_copy(a, b, load_sem.at[k]) for k, (a, b) in enumerate(
        ((order_hbm, order_ref), (samples_hbm, samples), (skel_hbm, skel_ref)))]
    for load in loads:
        load.start()
    number = iter(range(56))

    def send(source, target, d):
        i = next(number)
        copy = pltpu.make_async_remote_copy(
            src_ref=source, dst_ref=target, send_sem=out_sem.at[i], recv_sem=in_sem.at[i],
            device_id={"row": around(d)}, device_id_type=pl.DeviceIdType.MESH)
        copy.start()
        return copy

    lead, rest, upper, lower = [Stream(me, send, *streams[6 * k:6 * k + 6]) for k in range(4)]
    big[...] = jnp.zeros_like(big)
    loads[0].wait()
    place = lax.broadcasted_iota(jnp.int32, (cols, cols), 0)
    move = jnp.where(place == order_ref[...], 1.0, 0.0).astype(BF16)
    loads[1].wait()
    xp_ref[...] = mul(samples[...], move, NN, False).astype(BF16)
    xp = xp_ref[...]
    parts = [
        [mul(xp[:, i * BLOCK:(i + 1) * BLOCK], xp[:, i * BLOCK:], TN, False)[:, j * BLOCK:(j + 1) * BLOCK]
         for j in range(n - i)] for i in range(n)
    ]
    one, two = fold(parts[1][0], parts[0][0], parts[2][0])
    lead.put(0, one)
    for b, value in enumerate((two, parts[0][1], parts[0][2], parts[1][1])):
        rest.put(b, value)
    pl.semaphore_wait(barrier, len(partners))
    lead.spread()
    rest.spread()

    def tell(k, steps):
        for d in steps:
            pl.semaphore_signal(
                known.at[k], inc=1, device_id={"row": around(d)}, device_id_type=pl.DeviceIdType.MESH)

    tell(0, (2, -2))

    loads[2].wait()
    at = lax.broadcasted_iota(jnp.int32, (rows, keys), 0) + me * rows
    pick = jnp.where(at == skel_ref[...], 1.0, 0.0).astype(BF16)
    chosen = mul(pick, xp, TN, False)
    for half, stream in enumerate((upper, lower)):
        for j in range(n):
            stream.put(j, chosen[half * BLOCK:(half + 1) * BLOCK, j * BLOCK:(j + 1) * BLOCK])
    pl.semaphore_wait(known.at[0], 2)
    tell(1, (4, -4))
    pl.semaphore_wait(known.at[1], 2)
    lead.reduce_near()
    rest.reduce_near()
    upper.spread()
    lower.spread()
    lead.reduce_far()
    rest.reduce_far()
    upper.reduce_near()
    lower.reduce_near()
    lead.hand_back()
    rest.hand_back()
    upper.reduce_far()
    lower.reduce_far()

    scale = 1.0 / (rows * RING)
    r, c = places()
    lead.arrive()
    big[:BLOCK, :BLOCK] = jnp.where(r <= c, lead.get(0) * scale, 0.0)

    def go_on(j):
        if j == 0:
            rest.arrive()
            first, _, third = unfold(lead.get(0), rest.get(0))
            for (i, j), value in zip(
                    ((1, 1), (2, 2), (0, 1), (0, 2), (1, 2)),
                    (first, third, rest.get(1), rest.get(2), rest.get(3))):
                big[i * BLOCK:(i + 1) * BLOCK, j * BLOCK:(j + 1) * BLOCK] = value * scale
            upper.hand_back()
        elif j == 1:
            lower.hand_back()

    eliminate(big, n, work, inverse, between=go_on)
    e = big[:, cols:]
    e_high, e_low = pair(e)
    little[...] = jnp.zeros_like(little)

    def meet(stream, half):
        stream.arrive()
        some = jnp.concatenate([stream.get(j) for j in range(n)], axis=1)
        picked = pl.ds(half * BLOCK, BLOCK)
        solved[picked, :] = mul(some, e, NT)
        return solved[picked, :]

    top = meet(upper, 0)
    little[:BLOCK, :BLOCK] = mul(top, top, NT)

    def second(j):
        if j == 0:
            low = meet(lower, 1)
            little[:BLOCK, BLOCK:keys] = mul(solved[:BLOCK, :], low, NT)
            little[BLOCK:, BLOCK:keys] = mul(low, low, NT)

    few = rows // m // 4

    def slice_of_q(j, step):
        part = pl.ds(pl.multiple_of((j * 4 + step) * few, few), few)
        x = xp_ref[part, :]
        value = mul(x, e_high, NT, False) + mul(x, e_low, NT, False)
        q_ref[part, :] = value
        high, low = pair(value)
        high_ref[part, :] = high
        low_ref[part, :] = low

    eliminate(little, m, work, inverse, right=solved, between=second, beside=slice_of_q)
    right_ref[...] = mul(little[:, keys:], solved[...], TN)
    for stream in (lead, rest, upper, lower):
        stream.drain()


def on_device(samples, column_order, skeleton):
    _, rows, cols = samples.shape
    keys = skeleton.shape[1]
    n, m = cols // BLOCK, keys // BLOCK
    whole = pl.BlockSpec(memory_space=VMEM)
    outside = pl.BlockSpec(memory_space=pltpu.HBM)
    shape = jax.ShapeDtypeStruct
    q, high, low, right = pl.pallas_call(
        factor,
        out_shape=(
            shape((rows, cols), F32), shape((rows, cols), BF16), shape((rows, cols), BF16), shape((keys, cols), F32)),
        in_specs=[outside] * 3,
        out_specs=(whole,) * 4,
        scratch_shapes=room_of(1) + room_of(n * (n + 1) // 2 - 2) + room_of(n) * m + [
            VMEM((cols, 2 * cols), F32), VMEM((keys, 2 * keys), F32), VMEM((keys, cols), F32),
            VMEM((rows, cols), BF16), VMEM((rows, cols), BF16),
            VMEM((1, cols), jnp.int32), VMEM((1, keys), jnp.int32),
            VMEM((BLOCK + PANEL, 2 * BLOCK), F32), VMEM((BLOCK, BLOCK), F32),
        ] + [pltpu.SemaphoreType.DMA((56,))] * 2 + [pltpu.SemaphoreType.DMA((3,)), pltpu.SemaphoreType.REGULAR((2,))],
        compiler_params=pltpu.CompilerParams(
            collective_id=0, has_side_effects=True, vmem_limit_bytes=24 * 2 ** 20),
    )(*[pltpu.with_memory_space_constraint(v, pltpu.HBM) for v in (samples[0], column_order, skeleton)])
    q_factor, interp = pl.pallas_call(
        finish,
        out_shape=(shape((rows, cols), F32), shape((rows, keys), BF16)),
        in_specs=[whole] * 4,
        out_specs=(outside, outside),
        scratch_shapes=[VMEM((rows, keys), BF16), pltpu.SemaphoreType.DMA((5,))],
        compiler_params=pltpu.CompilerParams(vmem_limit_bytes=16 * 2 ** 20),
    )(q, high, low, right)
    return q_factor[None], interp[None]


def solution(mesh):
    placed = (P("node", "row", None), P("node", None), P("node", None))
    return jax.shard_map(
        on_device,
        mesh=mesh,
        in_specs=placed,
        out_specs=(P("node", "row", None), P("node", "row", None)),
        check_vma=False,
    )
```

```python
import functools

import jax
import jax.numpy as jnp
from jax import lax
from jax.experimental import pallas as pl
from jax.experimental.pallas import tpu as pltpu
from jax.sharding import PartitionSpec as P

F32, BF16 = jnp.float32, jnp.bfloat16
BLOCK = 128
PANEL = 8
RING = 16
VMEM = pltpu.VMEM


def split(x):
    high = x.astype(BF16).astype(F32)
    rest = x - high
    mid = rest.astype(BF16).astype(F32)
    return high, mid, rest - mid


def pair(x):
    high = x.astype(BF16)
    return high, (x - high.astype(F32)).astype(BF16)


def mul(a, b, dims, exact=True):
    if exact:
        left, right = split(a), split(b)
        a = jnp.concatenate([left[i].astype(BF16) for i in (0, 0, 1, 0, 1, 2)], axis=dims[0][0])
        b = jnp.concatenate([right[i].astype(BF16) for i in (0, 1, 0, 2, 1, 0)], axis=dims[1][0])
    return lax.dot_general(a, b, (dims, ((), ())), preferred_element_type=F32)


NN, NT, TN = ((1,), (0,)), ((1,), (1,)), ((0,), (0,))


def row(x, k):
    return jnp.broadcast_to(x[k:k + 1], x.shape)


def take(x, index):
    return jnp.take_along_axis(x, index, axis=1)


def identity():
    r = lax.broadcasted_iota(jnp.int32, (BLOCK, BLOCK), 0)
    c = lax.broadcasted_iota(jnp.int32, (BLOCK, BLOCK), 1)
    return jnp.where(r == c, 1.0, 0.0).astype(F32)


def invert_block(work, inverse, beside=None):
    sub = lax.broadcasted_iota(jnp.int32, (PANEL, BLOCK), 0)
    lane = lax.broadcasted_iota(jnp.int32, (PANEL, BLOCK), 1)

    def panel(p, carry):
        here_a, here_e, last_a, last_e = carry
        base = pl.multiple_of(PANEL * p, PANEL)
        at = sub + base
        after = (at + PANEL) & (BLOCK - 1)
        left = split(jnp.where(lane >= base + 2 * PANEL, last_a, 0.0))
        right = split(jnp.concatenate([last_a, last_e], axis=1))
        lhs = jnp.concatenate([left[i] for i in (0, 0, 1, 0, 1, 2)], axis=0).astype(BF16)
        rhs = jnp.concatenate([right[i] for i in (0, 1, 0, 2, 1, 0)], axis=0).astype(BF16)
        next_a = work[pl.ds(base + PANEL, PANEL), :BLOCK]
        next_e = work[pl.ds(base + PANEL, PANEL), BLOCK:]
        work[:BLOCK, :] = work[:BLOCK, :] - mul(lhs, rhs, TN, exact=False)
        for k in range(PANEL):
            coef = take(row(last_a, k), after)
            next_a = next_a - coef * row(last_a, k)
            next_e = next_e - coef * row(last_e, k)
        own = [take(row(here_a, k), at) for k in range(PANEL)]
        down = [take(row(here_a, k), after) for k in range(PANEL)]
        for k in range(PANEL):
            scale = lax.rsqrt(row(own[k], k))
            lo, ln = own[k] * scale, down[k] * scale
            for m in range(k + 1, PANEL):
                s = row(lo, m)
                own[m] = own[m] - lo * s
                down[m] = down[m] - ln * s
            ua, ue = row(here_a, k) * scale, row(here_e, k) * scale
            below = jnp.where(sub > k, lo, 0.0)
            here_a = jnp.where(sub == k, ua, here_a - below * ua)
            here_e = jnp.where(sub == k, ue, here_e - below * ue)
            next_a = next_a - ln * ua
            next_e = next_e - ln * ue
        inverse[pl.ds(base, PANEL), :] = here_e
        return next_a, next_e, here_a, here_e

    def several(step, carry):
        if beside is not None:
            beside(step)
        for k in range(4):
            carry = panel(step * 4 + k, carry)
        return carry

    zero = jnp.zeros((PANEL, BLOCK), F32)
    first = (work[:PANEL, :BLOCK], work[:PANEL, BLOCK:], zero, zero)
    lax.fori_loop(0, BLOCK // PANEL // 4, several, first)


def eliminate(both, n, work, inverse, right=None, between=None, beside=None):
    half = n * BLOCK
    work[BLOCK:, :] = jnp.zeros((PANEL, 2 * BLOCK), F32)
    for j in range(n):
        rows = pl.ds(j * BLOCK, BLOCK)
        work[:BLOCK, :BLOCK] = both[rows, j * BLOCK:(j + 1) * BLOCK]
        work[:BLOCK, BLOCK:] = identity()
        invert_block(work, inverse, functools.partial(beside, j) if beside is not None else None)
        if between is not None:
            between(j)
        w = inverse[...]
        first, end = (j + 1) * BLOCK, half + j * BLOCK
        both[rows, first:end] = mul(w, both[rows, first:end], NN)
        both[rows, end:end + BLOCK] = w
        if right is not None:
            right[rows, :] = mul(w, right[rows, :], NN)
        for i in range(j + 1, n):
            lead = both[rows, i * BLOCK:(i + 1) * BLOCK]
            below = pl.ds(i * BLOCK, BLOCK)
            span = slice(i * BLOCK, end + BLOCK)
            both[below, span] = both[below, span] - mul(lead, both[rows, span], TN)
            if right is not None:
                right[below, :] = right[below, :] - mul(lead, right[rows, :], TN)


def finish(q_ref, high_ref, low_ref, right_ref, q_out, interp_out, interp, sems):
    whole_q = pltpu.make_async_copy(q_ref, q_out, sems.at[0])
    whole_q.start()
    r_high, r_low = pair(right_ref[...])
    size = q_ref.shape[0] // 4
    copies = []
    for step in range(4):
        rows = pl.ds(step * size, size)
        high, low = high_ref[rows, :], low_ref[rows, :]
        out = mul(high, r_high, NT, False) + mul(low, r_high, NT, False) + mul(high, r_low, NT, False)
        interp[rows, :] = out.astype(BF16)
        copies.append(pltpu.make_async_copy(interp.at[rows, :], interp_out.at[rows, :], sems.at[1 + step]))
        copies[-1].start()
    whole_q.wait()
    for copy in copies:
        copy.wait()


def places():
    r = lax.broadcasted_iota(jnp.int32, (BLOCK, BLOCK), 0)
    c = lax.broadcasted_iota(jnp.int32, (BLOCK, BLOCK), 1)
    return r, c


def fold(first, second, third):
    r, c = places()
    edge = jnp.sum(jnp.where(r == c, first, 0.0), axis=0, keepdims=True)
    corner = first[BLOCK - 1:, BLOCK - 1:]
    one = jnp.where(r > c, first, second)
    two = jnp.where(r == c + 1, edge, third)
    return one, jnp.where((r == BLOCK - 1) & (c == 0), corner, two)


def unfold(one, two):
    r, c = places()
    edge = jnp.sum(jnp.where(r == c + 1, two, 0.0), axis=0, keepdims=True)
    corner = two[BLOCK - 1:, :1]
    edge = jnp.where(c == BLOCK - 1, corner, edge)
    first = jnp.where(r < c, one.T, jnp.where(r == c, edge, 0.0))
    return first, jnp.where(r <= c, one, 0.0), jnp.where(r <= c, two, 0.0)


class Stream:
    def __init__(self, me, send, mine, near, edge, part, mate, full):
        self.me, self.send = me, send
        self.mine, self.near, self.edge = mine, near, edge
        self.part, self.mate, self.full = part, mate, full
        self.residue, self.quarter = lax.rem(me, 4), lax.div(me, 4)
        self.sent, self.due = [], []

    def begin(self, copies):
        self.due = copies
        self.sent += copies

    def arrive(self):
        for copy in self.due:
            copy.wait_recv()

    def put(self, b, value):
        value = value.reshape(4, 4, PANEL, BLOCK)
        for k in range(4):
            self.mine[k, :, b * PANEL:(b + 1) * PANEL, :] = value[:, k]

    def get(self, b):
        value = jnp.stack([self.full[k, :, b * PANEL:(b + 1) * PANEL, :] for k in range(4)], axis=1)
        return value.reshape(BLOCK, BLOCK)

    def spread(self):
        self.begin(
            [self.send(self.mine.at[lax.rem(self.me + 2, 4), pl.ds(h, 2)], self.edge.at[pl.ds(h, 2)], d)
             for d, h in ((2, 0), (-2, 2))]
            + [self.send(self.mine.at[lax.rem(self.me + d + RING, 4)], self.near.at[k], d)
               for k, d in enumerate((1, -1))])

    def reduce_near(self):
        self.arrive()
        self.part[...] = (self.mine[self.residue] + self.edge[...]) + (self.near[0] + self.near[1])
        self.begin([self.send(self.part.at[lax.rem(self.quarter + (d // 4 + 4), 4)], self.mate.at[k], d)
                    for k, d in enumerate((8, 4, -4))])

    def reduce_far(self):
        self.arrive()
        own = self.full.at[self.residue, self.quarter]
        own[...] = (self.part[self.quarter] + self.mate[0]) + (self.mate[1] + self.mate[2])
        self.begin([self.send(own, own, d) for d in (8, 4, -4)])

    def hand_back(self):
        self.arrive()
        piece = lambda h: self.full.at[self.residue, pl.ds(h, 2)]
        self.begin([self.send(piece(h), piece(h), d) for d, h in ((2, 0), (-2, 2))]
                   + [self.send(self.full.at[self.residue], self.full.at[self.residue], d) for d in (1, -1)])

    def drain(self):
        for copy in self.sent:
            copy.wait_send()


def room_of(blocks):
    rows = blocks * PANEL
    return [VMEM(shape + (rows, BLOCK), F32) for shape in ((4, 4), (2, 4), (4,), (4,), (3,), (4, 4))]


def factor(samples_hbm, order_hbm, skel_hbm, q_ref, high_ref, low_ref, right_ref, *scratch):
    streams = scratch[:24]
    (big, little, solved, samples, xp_ref, order_ref, skel_ref, work, inverse, out_sem, in_sem, load_sem, known) = scratch[24:]
    me = lax.axis_index("row")
    rows, cols = samples.shape
    keys = skel_ref.shape[1]
    n, m = cols // BLOCK, keys // BLOCK
    around = lambda d: lax.rem(me + (d + RING), RING)
    barrier = pltpu.get_barrier_semaphore()
    partners = (2, -2, 1, -1)
    for d in partners:
        pl.semaphore_signal(
            barrier, inc=1, device_id={"row": around(d)}, device_id_type=pl.DeviceIdType.MESH)
    loads = [pltpu.make_async_copy(a, b, load_sem.at[k]) for k, (a, b) in enumerate(
        ((order_hbm, order_ref), (samples_hbm, samples), (skel_hbm, skel_ref)))]
    for load in loads:
        load.start()
    number = iter(range(56))

    def send(source, target, d):
        i = next(number)
        copy = pltpu.make_async_remote_copy(
            src_ref=source, dst_ref=target, send_sem=out_sem.at[i], recv_sem=in_sem.at[i],
            device_id={"row": around(d)}, device_id_type=pl.DeviceIdType.MESH)
        copy.start()
        return copy

    lead, rest, upper, lower = [Stream(me, send, *streams[6 * k:6 * k + 6]) for k in range(4)]
    big[...] = jnp.zeros_like(big)
    loads[0].wait()
    place = lax.broadcasted_iota(jnp.int32, (cols, cols), 0)
    move = jnp.where(place == order_ref[...], 1.0, 0.0).astype(BF16)
    loads[1].wait()
    xp_ref[...] = mul(samples[...], move, NN, False).astype(BF16)
    xp = xp_ref[...]
    parts = [
        [mul(xp[:, i * BLOCK:(i + 1) * BLOCK], xp[:, i * BLOCK:], TN, False)[:, j * BLOCK:(j + 1) * BLOCK]
         for j in range(n - i)] for i in range(n)
    ]
    one, two = fold(parts[1][0], parts[0][0], parts[2][0])
    lead.put(0, one)
    for b, value in enumerate((two, parts[0][1], parts[0][2], parts[1][1])):
        rest.put(b, value)
    pl.semaphore_wait(barrier, len(partners))
    lead.spread()
    rest.spread()

    def tell(k, steps):
        for d in steps:
            pl.semaphore_signal(
                known.at[k], inc=1, device_id={"row": around(d)}, device_id_type=pl.DeviceIdType.MESH)

    tell(0, (2, -2))

    loads[2].wait()
    at = lax.broadcasted_iota(jnp.int32, (rows, keys), 0) + me * rows
    pick = jnp.where(at == skel_ref[...], 1.0, 0.0).astype(BF16)
    chosen = mul(pick, xp, TN, False)
    for half, stream in enumerate((upper, lower)):
        for j in range(n):
            stream.put(j, chosen[half * BLOCK:(half + 1) * BLOCK, j * BLOCK:(j + 1) * BLOCK])
    upper.spread()
    pl.semaphore_wait(known.at[0], 2)
    tell(1, (4, -4))
    pl.semaphore_wait(known.at[1], 2)
    lead.reduce_near()
    rest.reduce_near()
    lower.spread()
    lead.reduce_far()
    rest.reduce_far()
    upper.reduce_near()
    lower.reduce_near()
    lead.hand_back()
    rest.hand_back()
    upper.reduce_far()
    lower.reduce_far()

    scale = 1.0 / (rows * RING)
    r, c = places()
    lead.arrive()
    big[:BLOCK, :BLOCK] = jnp.where(r <= c, lead.get(0) * scale, 0.0)

    def go_on(j):
        if j == 0:
            rest.arrive()
            first, _, third = unfold(lead.get(0), rest.get(0))
            for (i, j), value in zip(
                    ((1, 1), (2, 2), (0, 1), (0, 2), (1, 2)),
                    (first, third, rest.get(1), rest.get(2), rest.get(3))):
                big[i * BLOCK:(i + 1) * BLOCK, j * BLOCK:(j + 1) * BLOCK] = value * scale
            upper.hand_back()
        elif j == 1:
            lower.hand_back()

    eliminate(big, n, work, inverse, between=go_on)
    e = big[:, cols:]
    e_high, e_low = pair(e)
    little[...] = jnp.zeros_like(little)

    def meet(stream, half):
        stream.arrive()
        some = jnp.concatenate([stream.get(j) for j in range(n)], axis=1)
        picked = pl.ds(half * BLOCK, BLOCK)
        solved[picked, :] = mul(some, e, NT)
        return solved[picked, :]

    top = meet(upper, 0)
    little[:BLOCK, :BLOCK] = mul(top, top, NT)

    def second(j):
        if j == 0:
            low = meet(lower, 1)
            little[:BLOCK, BLOCK:keys] = mul(solved[:BLOCK, :], low, NT)
            little[BLOCK:, BLOCK:keys] = mul(low, low, NT)

    few = rows // m // 4

    def slice_of_q(j, step):
        part = pl.ds(pl.multiple_of((j * 4 + step) * few, few), few)
        x = xp_ref[part, :]
        value = mul(x, e_high, NT, False) + mul(x, e_low, NT, False)
        q_ref[part, :] = value
        high, low = pair(value)
        high_ref[part, :] = high
        low_ref[part, :] = low

    eliminate(little, m, work, inverse, right=solved, between=second, beside=slice_of_q)
    right_ref[...] = mul(little[:, keys:], solved[...], TN)
    for stream in (lead, rest, upper, lower):
        stream.drain()


def on_device(samples, column_order, skeleton):
    _, rows, cols = samples.shape
    keys = skeleton.shape[1]
    n, m = cols // BLOCK, keys // BLOCK
    whole = pl.BlockSpec(memory_space=VMEM)
    outside = pl.BlockSpec(memory_space=pltpu.HBM)
    shape = jax.ShapeDtypeStruct
    q, high, low, right = pl.pallas_call(
        factor,
        out_shape=(
            shape((rows, cols), F32), shape((rows, cols), BF16), shape((rows, cols), BF16), shape((keys, cols), F32)),
        in_specs=[outside] * 3,
        out_specs=(whole,) * 4,
        scratch_shapes=room_of(1) + room_of(n * (n + 1) // 2 - 2) + room_of(n) * m + [
            VMEM((cols, 2 * cols), F32), VMEM((keys, 2 * keys), F32), VMEM((keys, cols), F32),
            VMEM((rows, cols), BF16), VMEM((rows, cols), BF16),
            VMEM((1, cols), jnp.int32), VMEM((1, keys), jnp.int32),
            VMEM((BLOCK + PANEL, 2 * BLOCK), F32), VMEM((BLOCK, BLOCK), F32),
        ] + [pltpu.SemaphoreType.DMA((56,))] * 2 + [pltpu.SemaphoreType.DMA((3,)), pltpu.SemaphoreType.REGULAR((2,))],
        compiler_params=pltpu.CompilerParams(
            collective_id=0, has_side_effects=True, vmem_limit_bytes=24 * 2 ** 20),
    )(*[pltpu.with_memory_space_constraint(v, pltpu.HBM) for v in (samples[0], column_order, skeleton)])
    q_factor, interp = pl.pallas_call(
        finish,
        out_shape=(shape((rows, cols), F32), shape((rows, keys), BF16)),
        in_specs=[whole] * 4,
        out_specs=(outside, outside),
        scratch_shapes=[VMEM((rows, keys), BF16), pltpu.SemaphoreType.DMA((5,))],
        compiler_params=pltpu.CompilerParams(vmem_limit_bytes=16 * 2 ** 20),
    )(q, high, low, right)
    return q_factor[None], interp[None]


def solution(mesh):
    placed = (P("node", "row", None), P("node", None), P("node", None))
    return jax.shard_map(
        on_device,
        mesh=mesh,
        in_specs=placed,
        out_specs=(P("node", "row", None), P("node", "row", None)),
        check_vma=False,
    )
```

```python
import functools

import jax
import jax.numpy as jnp
from jax import lax
from jax.experimental import pallas as pl
from jax.experimental.pallas import tpu as pltpu
from jax.sharding import PartitionSpec as P

F32, BF16 = jnp.float32, jnp.bfloat16
BLOCK = 128
PANEL = 8
RING = 16
VMEM = pltpu.VMEM


def split(x):
    high = x.astype(BF16).astype(F32)
    rest = x - high
    mid = rest.astype(BF16).astype(F32)
    return high, mid, rest - mid


def pair(x):
    high = x.astype(BF16)
    return high, (x - high.astype(F32)).astype(BF16)


def mul(a, b, dims, exact=True):
    if exact:
        left, right = split(a), split(b)
        a = jnp.concatenate([left[i].astype(BF16) for i in (0, 0, 1, 0, 1, 2)], axis=dims[0][0])
        b = jnp.concatenate([right[i].astype(BF16) for i in (0, 1, 0, 2, 1, 0)], axis=dims[1][0])
    return lax.dot_general(a, b, (dims, ((), ())), preferred_element_type=F32)


NN, NT, TN = ((1,), (0,)), ((1,), (1,)), ((0,), (0,))


def row(x, k):
    return jnp.broadcast_to(x[k:k + 1], x.shape)


def take(x, index):
    return jnp.take_along_axis(x, index, axis=1)


def identity():
    r = lax.broadcasted_iota(jnp.int32, (BLOCK, BLOCK), 0)
    c = lax.broadcasted_iota(jnp.int32, (BLOCK, BLOCK), 1)
    return jnp.where(r == c, 1.0, 0.0).astype(F32)


def invert_block(work, inverse, beside=None):
    sub = lax.broadcasted_iota(jnp.int32, (PANEL, BLOCK), 0)
    lane = lax.broadcasted_iota(jnp.int32, (PANEL, BLOCK), 1)

    def panel(p, carry):
        here_a, here_e, last_a, last_e, own, coef = carry
        own, far = list(own), []
        base = pl.multiple_of(PANEL * p, PANEL)
        at = sub + base
        after = (at + PANEL) & (BLOCK - 1)
        left = split(jnp.where(lane >= base + 2 * PANEL, last_a, 0.0))
        right = split(jnp.concatenate([last_a, last_e], axis=1))
        lhs = jnp.concatenate([left[i] for i in (0, 0, 1, 0, 1, 2)], axis=0).astype(BF16)
        rhs = jnp.concatenate([right[i] for i in (0, 1, 0, 2, 1, 0)], axis=0).astype(BF16)
        next_a = work[pl.ds(base + PANEL, PANEL), :BLOCK]
        next_e = work[pl.ds(base + PANEL, PANEL), BLOCK:]
        work[:BLOCK, :] = work[:BLOCK, :] - mul(lhs, rhs, TN, exact=False)
        for k in range(PANEL):
            next_a = next_a - coef[k] * row(last_a, k)
            next_e = next_e - coef[k] * row(last_e, k)
        down = [take(row(here_a, k), after) for k in range(PANEL)]
        ahead = [take(row(next_a, k), after) for k in range(PANEL)]
        beyond = [take(row(here_a, k), (at + 2 * PANEL) & (BLOCK - 1)) for k in range(PANEL)]
        for k in range(PANEL):
            scale = lax.rsqrt(row(own[k], k))
            lo, ln, lb = own[k] * scale, down[k] * scale, beyond[k] * scale
            far.append(lb)
            for m in range(k + 1, PANEL):
                s = row(lo, m)
                own[m] = own[m] - lo * s
                down[m] = down[m] - ln * s
                beyond[m] = beyond[m] - lb * s
            ua, ue = row(here_a, k) * scale, row(here_e, k) * scale
            below = jnp.where(sub > k, lo, 0.0)
            here_a = jnp.where(sub == k, ua, here_a - below * ua)
            here_e = jnp.where(sub == k, ue, here_e - below * ue)
            next_a = next_a - ln * ua
            next_e = next_e - ln * ue
            for m in range(PANEL):
                ahead[m] = ahead[m] - ln * row(ln, m)
        inverse[pl.ds(base, PANEL), :] = here_e
        return next_a, next_e, here_a, here_e, tuple(ahead), tuple(far)

    def several(step, carry):
        for part in range(2):
            if beside is not None:
                beside(step * 2 + part)
            for k in range(4):
                carry = panel((step * 2 + part) * 4 + k, carry)
        return carry

    zero = jnp.zeros((PANEL, BLOCK), F32)
    top = work[:PANEL, :BLOCK]
    start = tuple(take(row(top, k), sub) for k in range(PANEL))
    first = (top, work[:PANEL, BLOCK:], zero, zero, start, (zero,) * PANEL)
    lax.fori_loop(0, BLOCK // PANEL // 8, several, first)


def eliminate(both, n, work, inverse, right=None, between=None, beside=None):
    half = n * BLOCK
    work[BLOCK:, :] = jnp.zeros((PANEL, 2 * BLOCK), F32)
    for j in range(n):
        rows = pl.ds(j * BLOCK, BLOCK)
        work[:BLOCK, :BLOCK] = both[rows, j * BLOCK:(j + 1) * BLOCK]
        work[:BLOCK, BLOCK:] = identity()
        invert_block(work, inverse, functools.partial(beside, j) if beside is not None else None)
        if between is not None:
            between(j)
        w = inverse[...]
        first, end = (j + 1) * BLOCK, half + j * BLOCK
        both[rows, first:end] = mul(w, both[rows, first:end], NN)
        both[rows, end:end + BLOCK] = w
        if right is not None:
            right[rows, :] = mul(w, right[rows, :], NN)
        for i in range(j + 1, n):
            lead = both[rows, i * BLOCK:(i + 1) * BLOCK]
            below = pl.ds(i * BLOCK, BLOCK)
            span = slice(i * BLOCK, end + BLOCK)
            both[below, span] = both[below, span] - mul(lead, both[rows, span], TN)
            if right is not None:
                right[below, :] = right[below, :] - mul(lead, right[rows, :], TN)


def finish(q_ref, high_ref, low_ref, right_ref, q_out, interp_out, interp, sems):
    whole_q = pltpu.make_async_copy(q_ref, q_out, sems.at[0])
    whole_q.start()
    r_high, r_low = pair(right_ref[...])
    size = q_ref.shape[0] // 4
    copies = []
    for step in range(4):
        rows = pl.ds(step * size, size)
        high, low = high_ref[rows, :], low_ref[rows, :]
        out = mul(high, r_high, NT, False) + mul(low, r_high, NT, False) + mul(high, r_low, NT, False)
        interp[rows, :] = out.astype(BF16)
        copies.append(pltpu.make_async_copy(interp.at[rows, :], interp_out.at[rows, :], sems.at[1 + step]))
        copies[-1].start()
    whole_q.wait()
    for copy in copies:
        copy.wait()


def places():
    r = lax.broadcasted_iota(jnp.int32, (BLOCK, BLOCK), 0)
    c = lax.broadcasted_iota(jnp.int32, (BLOCK, BLOCK), 1)
    return r, c


def fold(first, second, third):
    r, c = places()
    edge = jnp.sum(jnp.where(r == c, first, 0.0), axis=0, keepdims=True)
    corner = first[BLOCK - 1:, BLOCK - 1:]
    one = jnp.where(r > c, first, second)
    two = jnp.where(r == c + 1, edge, third)
    return one, jnp.where((r == BLOCK - 1) & (c == 0), corner, two)


def unfold(one, two):
    r, c = places()
    edge = jnp.sum(jnp.where(r == c + 1, two, 0.0), axis=0, keepdims=True)
    corner = two[BLOCK - 1:, :1]
    edge = jnp.where(c == BLOCK - 1, corner, edge)
    first = jnp.where(r < c, one.T, jnp.where(r == c, edge, 0.0))
    return first, jnp.where(r <= c, one, 0.0), jnp.where(r <= c, two, 0.0)


class Stream:
    def __init__(self, me, send, mine, near, edge, part, mate, full):
        self.me, self.send = me, send
        self.mine, self.near, self.edge = mine, near, edge
        self.part, self.mate, self.full = part, mate, full
        self.residue, self.quarter = lax.rem(me, 4), lax.div(me, 4)
        self.sent, self.due = [], []

    def begin(self, copies):
        self.due = copies
        self.sent += copies

    def arrive(self):
        for copy in self.due:
            copy.wait_recv()

    def put(self, b, value):
        value = value.reshape(4, 4, PANEL, BLOCK)
        for k in range(4):
            self.mine[k, :, b * PANEL:(b + 1) * PANEL, :] = value[:, k]

    def get(self, b):
        value = jnp.stack([self.full[k, :, b * PANEL:(b + 1) * PANEL, :] for k in range(4)], axis=1)
        return value.reshape(BLOCK, BLOCK)

    def spread(self):
        self.begin(
            [self.send(self.mine.at[lax.rem(self.me + 2, 4), pl.ds(h, 2)], self.edge.at[pl.ds(h, 2)], d)
             for d, h in ((2, 0), (-2, 2))]
            + [self.send(self.mine.at[lax.rem(self.me + d + RING, 4)], self.near.at[k], d)
               for k, d in enumerate((1, -1))])

    def reduce_near(self):
        self.arrive()
        self.part[...] = (self.mine[self.residue] + self.edge[...]) + (self.near[0] + self.near[1])
        self.begin([self.send(self.part.at[lax.rem(self.quarter + (d // 4 + 4), 4)], self.mate.at[k], d)
                    for k, d in enumerate((8, 4, -4))])

    def reduce_far(self):
        self.arrive()
        own = self.full.at[self.residue, self.quarter]
        own[...] = (self.part[self.quarter] + self.mate[0]) + (self.mate[1] + self.mate[2])
        self.begin([self.send(own, own, d) for d in (8, 4, -4)])

    def hand_back(self):
        self.arrive()
        piece = lambda h: self.full.at[self.residue, pl.ds(h, 2)]
        self.begin([self.send(piece(h), piece(h), d) for d, h in ((2, 0), (-2, 2))]
                   + [self.send(self.full.at[self.residue], self.full.at[self.residue], d) for d in (1, -1)])

    def drain(self):
        for copy in self.sent:
            copy.wait_send()


def room_of(blocks):
    rows = blocks * PANEL
    return [VMEM(shape + (rows, BLOCK), F32) for shape in ((4, 4), (2, 4), (4,), (4,), (3,), (4, 4))]


def factor(samples_hbm, order_hbm, skel_hbm, q_ref, high_ref, low_ref, right_ref, *scratch):
    streams = scratch[:24]
    (big, little, solved, samples, xp_ref, order_ref, skel_ref, work, inverse, out_sem, in_sem, load_sem, known) = scratch[24:]
    me = lax.axis_index("row")
    rows, cols = samples.shape
    keys = skel_ref.shape[1]
    n, m = cols // BLOCK, keys // BLOCK
    around = lambda d: lax.rem(me + (d + RING), RING)
    barrier = pltpu.get_barrier_semaphore()
    partners = (2, -2, 1, -1)
    for d in partners:
        pl.semaphore_signal(
            barrier, inc=1, device_id={"row": around(d)}, device_id_type=pl.DeviceIdType.MESH)
    loads = [pltpu.make_async_copy(a, b, load_sem.at[k]) for k, (a, b) in enumerate(
        ((order_hbm, order_ref), (samples_hbm, samples), (skel_hbm, skel_ref)))]
    for load in loads:
        load.start()
    number = iter(range(56))

    def send(source, target, d):
        i = next(number)
        copy = pltpu.make_async_remote_copy(
            src_ref=source, dst_ref=target, send_sem=out_sem.at[i], recv_sem=in_sem.at[i],
            device_id={"row": around(d)}, device_id_type=pl.DeviceIdType.MESH)
        copy.start()
        return copy

    lead, rest, upper, lower = [Stream(me, send, *streams[6 * k:6 * k + 6]) for k in range(4)]
    big[...] = jnp.zeros_like(big)
    loads[0].wait()
    place = lax.broadcasted_iota(jnp.int32, (cols, cols), 0)
    move = jnp.where(place == order_ref[...], 1.0, 0.0).astype(BF16)
    loads[1].wait()
    xp_ref[...] = mul(samples[...], move, NN, False).astype(BF16)
    xp = xp_ref[...]
    parts = [
        [mul(xp[:, i * BLOCK:(i + 1) * BLOCK], xp[:, i * BLOCK:], TN, False)[:, j * BLOCK:(j + 1) * BLOCK]
         for j in range(n - i)] for i in range(n)
    ]
    one, two = fold(parts[1][0], parts[0][0], parts[2][0])
    lead.put(0, one)
    for b, value in enumerate((two, parts[0][1], parts[0][2], parts[1][1])):
        rest.put(b, value)
    pl.semaphore_wait(barrier, len(partners))
    lead.spread()
    rest.spread()

    def tell(k, steps):
        for d in steps:
            pl.semaphore_signal(
                known.at[k], inc=1, device_id={"row": around(d)}, device_id_type=pl.DeviceIdType.MESH)

    tell(0, (2, -2))

    loads[2].wait()
    at = lax.broadcasted_iota(jnp.int32, (rows, keys), 0) + me * rows
    pick = jnp.where(at == skel_ref[...], 1.0, 0.0).astype(BF16)
    chosen = mul(pick, xp, TN, False)
    for half, stream in enumerate((upper, lower)):
        for j in range(n):
            stream.put(j, chosen[half * BLOCK:(half + 1) * BLOCK, j * BLOCK:(j + 1) * BLOCK])
    upper.spread()
    pl.semaphore_wait(known.at[0], 2)
    tell(1, (4, -4))
    pl.semaphore_wait(known.at[1], 2)
    lead.reduce_near()
    rest.reduce_near()
    lower.spread()
    lead.reduce_far()
    rest.reduce_far()
    upper.reduce_near()
    lower.reduce_near()
    lead.hand_back()
    rest.hand_back()
    upper.reduce_far()
    lower.reduce_far()

    scale = 1.0 / (rows * RING)
    r, c = places()
    lead.arrive()
    big[:BLOCK, :BLOCK] = jnp.where(r <= c, lead.get(0) * scale, 0.0)

    def go_on(j):
        if j == 0:
            rest.arrive()
            first, _, third = unfold(lead.get(0), rest.get(0))
            for (i, j), value in zip(
                    ((1, 1), (2, 2), (0, 1), (0, 2), (1, 2)),
                    (first, third, rest.get(1), rest.get(2), rest.get(3))):
                big[i * BLOCK:(i + 1) * BLOCK, j * BLOCK:(j + 1) * BLOCK] = value * scale
            upper.hand_back()
        elif j == 1:
            lower.hand_back()

    eliminate(big, n, work, inverse, between=go_on)
    e = big[:, cols:]
    e_high, e_low = pair(e)
    little[...] = jnp.zeros_like(little)

    def meet(stream, half):
        stream.arrive()
        some = jnp.concatenate([stream.get(j) for j in range(n)], axis=1)
        picked = pl.ds(half * BLOCK, BLOCK)
        solved[picked, :] = mul(some, e, NT)
        return solved[picked, :]

    top = meet(upper, 0)
    little[:BLOCK, :BLOCK] = mul(top, top, NT)

    def second(j):
        if j == 0:
            low = meet(lower, 1)
            little[:BLOCK, BLOCK:keys] = mul(solved[:BLOCK, :], low, NT)
            little[BLOCK:, BLOCK:keys] = mul(low, low, NT)

    few = rows // m // 4

    def slice_of_q(j, step):
        part = pl.ds(pl.multiple_of((j * 4 + step) * few, few), few)
        x = xp_ref[part, :]
        value = mul(x, e_high, NT, False) + mul(x, e_low, NT, False)
        q_ref[part, :] = value
        high, low = pair(value)
        high_ref[part, :] = high
        low_ref[part, :] = low

    eliminate(little, m, work, inverse, right=solved, between=second, beside=slice_of_q)
    right_ref[...] = mul(little[:, keys:], solved[...], TN)
    for stream in (lead, rest, upper, lower):
        stream.drain()


def on_device(samples, column_order, skeleton):
    _, rows, cols = samples.shape
    keys = skeleton.shape[1]
    n, m = cols // BLOCK, keys // BLOCK
    whole = pl.BlockSpec(memory_space=VMEM)
    outside = pl.BlockSpec(memory_space=pltpu.HBM)
    shape = jax.ShapeDtypeStruct
    q, high, low, right = pl.pallas_call(
        factor,
        out_shape=(
            shape((rows, cols), F32), shape((rows, cols), BF16), shape((rows, cols), BF16), shape((keys, cols), F32)),
        in_specs=[outside] * 3,
        out_specs=(whole,) * 4,
        scratch_shapes=room_of(1) + room_of(n * (n + 1) // 2 - 2) + room_of(n) * m + [
            VMEM((cols, 2 * cols), F32), VMEM((keys, 2 * keys), F32), VMEM((keys, cols), F32),
            VMEM((rows, cols), BF16), VMEM((rows, cols), BF16),
            VMEM((1, cols), jnp.int32), VMEM((1, keys), jnp.int32),
            VMEM((BLOCK + PANEL, 2 * BLOCK), F32), VMEM((BLOCK, BLOCK), F32),
        ] + [pltpu.SemaphoreType.DMA((56,))] * 2 + [pltpu.SemaphoreType.DMA((3,)), pltpu.SemaphoreType.REGULAR((2,))],
        compiler_params=pltpu.CompilerParams(
            collective_id=0, has_side_effects=True, vmem_limit_bytes=24 * 2 ** 20),
    )(*[pltpu.with_memory_space_constraint(v, pltpu.HBM) for v in (samples[0], column_order, skeleton)])
    q_factor, interp = pl.pallas_call(
        finish,
        out_shape=(shape((rows, cols), F32), shape((rows, keys), BF16)),
        in_specs=[whole] * 4,
        out_specs=(outside, outside),
        scratch_shapes=[VMEM((rows, keys), BF16), pltpu.SemaphoreType.DMA((5,))],
        compiler_params=pltpu.CompilerParams(vmem_limit_bytes=16 * 2 ** 20),
    )(q, high, low, right)
    return q_factor[None], interp[None]


def solution(mesh):
    placed = (P("node", "row", None), P("node", None), P("node", None))
    return jax.shard_map(
        on_device,
        mesh=mesh,
        in_specs=placed,
        out_specs=(P("node", "row", None), P("node", "row", None)),
        check_vma=False,
    )
```
